32 devices in a mesh: row: 4 (over x, core), col: 8 (over z, y).
Axes of the slice: x: 2, y: 2, z: 4, core: 2. Of those that a mesh axis runs over, the one named last changes fastest.
Arguments:
- dosage: bfloat16 [1536, 24576], P(None, ('row', 'col')), may hold values from 0 to 2
- zscores: bfloat16 [24576], P(('row', 'col')), may hold values from -18 to 18
- band_reach: int32 [32], replicated, may hold values from 0 to 2, as said below
Outputs:
- ld_tiles: bfloat16 [24576, 3840], P(('row', 'col'))
- smoothed: float32 [24576], P(('row', 'col'))
- quadratic: float32 [], replicated
The draws below stay inside these ranges and needn't reach their ends.
Inputs may be any that keep to these rules, and one draw needn't show every extreme that they name: `band_reach`: the first 3 blocks, the last 3 blocks and some two neighbouring blocks reach 2.
All inputs are finite; a program needn't handle non-finite values.
Results may differ from the reference program's by a relative error of at most 0.0042.
Values may be sent and summed in bfloat16 or wider, within the bound.
A program may use at most 64 MiB of HBM per device.

```python
import math
import jax
import jax.numpy as jnp
from jax import lax

BS = 768
NSAMP = 1536
BAND = 2
NBLOCKS = 32
SNPS = 24576
WIDE = 3840


def draw_dosage(key, part):
    key_freq, key_own = jax.random.split(key, 2)
    frequency = jnp.exp(jax.random.uniform(key_freq, (SNPS,), jnp.float32, math.log(0.05), math.log(0.5)))
    spread = jax.random.uniform(key_own, (NSAMP, SNPS), jnp.float32)
    mixed = spread
    return (4.0 * frequency[None, :] * mixed).astype(jnp.bfloat16)


def draw_zscores(key, part):
    position = jnp.arange(SNPS, dtype=jnp.float32) / (SNPS - 1)
    values = jnp.clip(jax.random.normal(key, (SNPS,), jnp.float32), -6.0, 6.0) * (1.0 + 2.0 * position)
    return values.astype(jnp.bfloat16)


def draw_band_reach(key, part):
    key_base = jax.random.fold_in(key, 11)
    key_place = jax.random.fold_in(key, 12)
    base = jax.random.randint(key_base, (NBLOCKS,), 0, BAND + 1, dtype=jnp.int32)
    place = jax.random.randint(key_place, (), 0, NBLOCKS - 1, dtype=jnp.int32)
    blocks = jnp.arange(NBLOCKS, dtype=jnp.int32)
    chosen = (blocks == place) | (blocks == place + 1)
    chosen = chosen | (blocks <= BAND) | (blocks >= NBLOCKS - 1 - BAND)
    return jnp.where(chosen, jnp.int32(BAND), base)


def setup_inputs(seed: int = 0) -> dict:
    key_list = jax.random.split(jax.random.key(seed), 4)
    dosage = draw_dosage(jax.random.fold_in(key_list[3], 71), 0)
    zscores = draw_zscores(jax.random.fold_in(key_list[3], 71), 0)
    band_reach = draw_band_reach(jax.random.fold_in(key_list[3], 71), 0)
    return {"dosage": dosage, "zscores": zscores, "band_reach": band_reach}


def standardize(dosage):
    values = dosage.astype(jnp.float32)
    column_mean = lax.optimization_barrier(jnp.mean(values, axis=0))
    centered = values - column_mean
    variance = lax.optimization_barrier(jnp.mean(centered * centered, axis=0))
    return (centered * lax.rsqrt(variance + 1e-05)).astype(jnp.bfloat16)

def reference(dosage, zscores, band_reach):
    scaled = standardize(dosage)
    margin = BAND * BS
    padded = jnp.pad(scaled, ((0, 0), (margin, margin)))
    padded_z = jnp.pad(zscores, (margin, margin))
    outside = jnp.full((BAND,), -1, jnp.int32)
    padded_reach = jnp.concatenate([outside, band_reach.astype(jnp.int32), outside])
    offsets = jnp.arange(-BAND, BAND + 1, dtype=jnp.int32)

    def one_block(block):
        start = (block * BS).astype(jnp.int32)
        own_block = lax.dynamic_slice_in_dim(scaled, start, BS, 1)
        near_block = lax.dynamic_slice_in_dim(padded, start, WIDE, 1)
        product = jnp.dot(own_block.T, near_block, preferred_element_type=jnp.float32) / NSAMP
        their_reach = lax.dynamic_slice_in_dim(padded_reach, block.astype(jnp.int32), 2 * BAND + 1, 0)
        own_reach = lax.dynamic_index_in_dim(band_reach, block.astype(jnp.int32), 0, False)
        allowed = (jnp.abs(offsets) <= jnp.minimum(own_reach, their_reach)).astype(jnp.float32)
        masked = product.reshape(BS, 2 * BAND + 1, BS) * allowed[None, :, None]
        tile_rows = masked.reshape(BS, WIDE).astype(jnp.bfloat16)
        near_z = lax.dynamic_slice_in_dim(padded_z, start, WIDE, 0)
        result = jnp.dot(tile_rows, near_z, preferred_element_type=jnp.float32)
        return (tile_rows, result)
    tiles, results = lax.map(one_block, jnp.arange(NBLOCKS, dtype=jnp.int32))
    ld_tiles = tiles.reshape(SNPS, WIDE)
    smoothed = results.reshape(SNPS)
    quadratic = jnp.sum(zscores.astype(jnp.float32) * smoothed) / SNPS
    return (ld_tiles, smoothed, quadratic)
```

```python
import jax
import jax.numpy as jnp
from jax import lax
from jax.sharding import PartitionSpec as P

BAND = 2
AXES = ("row", "col")
CHUNKS = 3


def standardize(dosage):
    values = dosage.astype(jnp.float32)
    column_mean = jnp.mean(values, axis=0)
    centered = values - column_mean
    variance = jnp.mean(centered * centered, axis=0)
    return (centered * lax.rsqrt(variance + 1e-05)).astype(jnp.bfloat16)


def body(dosage, zscores, band_reach):
    samples = dosage.shape[0]
    block_width = zscores.shape[0]
    block_count = lax.axis_size(AXES)
    position = lax.axis_index(AXES)
    even = position % 2 == 0
    width = block_width // CHUNKS

    swap = [(p, p ^ 1) for p in range(block_count)]
    out_hop = [(p, p - 2) for p in range(2, block_count, 2)]
    out_hop += [(p, p + 2) for p in range(1, block_count - 2, 2)]
    back_hop = [(b, a) for a, b in out_hop]

    def permute(value, pairs):
        return lax.ppermute(value, AXES, pairs)

    own_reach = lax.dynamic_index_in_dim(band_reach, position, 0, False)

    def allowed(offset):
        other = position + offset
        inside = (other >= 0) & (other < block_count)
        their_reach = lax.dynamic_index_in_dim(
            band_reach, jnp.clip(other, 0, block_count - 1), 0, False
        )
        return inside & (abs(offset) <= jnp.minimum(own_reach, their_reach))

    def gram(left, right):
        product = lax.dot_general(
            left, right, (((0,), (0,)), ((), ())), preferred_element_type=jnp.float32
        )
        return (product / samples).astype(jnp.bfloat16)

    pieces = [standardize(dosage[:, k * width : (k + 1) * width]) for k in range(CHUNKS)]
    far_pieces = [permute(piece, out_hop) for piece in pieces]
    partner_pieces = [permute(piece, swap) for piece in pieces]
    partner_z = permute(zscores, swap)
    far_z = permute(zscores, out_hop)
    back_z = permute(zscores, back_hop)
    back_partner_z = permute(far_z, swap)

    scaled = jnp.concatenate(pieces, axis=1)
    back = jnp.concatenate(
        [permute(gram(piece, scaled), back_hop) for piece in far_pieces], axis=0
    )
    partner = jnp.concatenate(partner_pieces, axis=1)
    back_partner = jnp.concatenate(
        [permute(gram(partner, piece), swap) for piece in far_pieces], axis=1
    )
    far_tile = jnp.concatenate([gram(scaled, piece) for piece in far_pieces], axis=1)
    partner_tile = gram(scaled, partner)
    own_tile = gram(scaled, scaled)

    def pick(offset, when_even, when_odd):
        chosen = jnp.where(even, when_even, when_odd)
        return jnp.where(allowed(offset), chosen, jnp.zeros_like(chosen))

    tiles = [
        pick(-2, back, far_tile),
        pick(-1, back_partner, partner_tile),
        own_tile,
        pick(1, partner_tile, back_partner),
        pick(2, far_tile, back),
    ]
    near_z = [
        jnp.where(even, back_z, far_z),
        jnp.where(even, back_partner_z, partner_z),
        zscores,
        jnp.where(even, partner_z, back_partner_z),
        jnp.where(even, far_z, back_z),
    ]
    ld_tiles = jnp.concatenate(tiles, axis=1)
    smoothed = jnp.dot(
        ld_tiles, jnp.concatenate(near_z), preferred_element_type=jnp.float32
    )
    total = lax.psum(jnp.sum(zscores.astype(jnp.float32) * smoothed), AXES)
    quadratic = total / (block_count * block_width)
    return (ld_tiles, smoothed, quadratic)


def solution(mesh):
    placed = (P(None, AXES), P(AXES), P())
    return jax.shard_map(
        body,
        mesh=mesh,
        in_specs=placed,
        out_specs=(P(AXES, None), P(AXES), P()),
        check_vma=False,
    )
```

```python
import functools

import jax
import jax.numpy as jnp
from jax import lax
from jax.experimental import pallas as pl
from jax.experimental.pallas import tpu as pltpu
from jax.sharding import PartitionSpec as P

BAND = 2
AXES = ("row", "col")
CHUNKS = 3
ZROWS = 16
MESH = pl.DeviceIdType.MESH


def standardize(chunk):
    values = chunk.astype(jnp.float32)
    column_mean = jnp.mean(values, axis=0, keepdims=True)
    centered = values - column_mean
    variance = jnp.mean(centered * centered, axis=0, keepdims=True)
    return (centered * lax.rsqrt(variance + 1e-05)).astype(jnp.bfloat16)


def kernel(
    rows, cols, flags, dosage, z_in, out, smooth, quad,
    raw, far_raw, part_raw, own, far, part, back_out, side_out, back_in, side_in,
    near_z, col_sums, row_sums, sum_out,
    local_sem, far_send, far_recv, part_send, part_recv, back_send, back_recv,
    side_send, side_recv, z_send, z_recv, col_send, col_recv, row_send, row_recv,
):
    samples, block = dosage.shape
    width = block // CHUNKS
    count = rows * cols
    row, col = lax.axis_index("row"), lax.axis_index("col")
    me = row * cols + col
    sign = 1 - 2 * (me % 2)

    def device(index):
        return (index // cols, index % cols)

    def present(index):
        return (index >= 0) & (index < count)

    onward, source, partner = me - 2 * sign, me + 2 * sign, me + sign
    has_onward, has_source = present(onward), present(source)
    offsets = (-2, -1, 1, 2)

    loads = []
    for k in range(CHUNKS):
        load = pltpu.make_async_copy(
            dosage.at[:, pl.ds(k * width, width)], raw.at[k], local_sem.at[k]
        )
        load.start()
        loads.append(load)
    near_z[...] = jnp.zeros_like(near_z)

    barrier = pltpu.get_barrier_semaphore()
    peers = cols - 1 + rows - 1
    for offset in offsets:
        outside = present(me + offset) & ((me + offset) // cols != row)
        peers = peers + jnp.where(outside, 1, 0)
        @pl.when(outside)
        def _():
            pl.semaphore_signal(
                barrier, inc=1, device_id=device(me + offset), device_id_type=MESH
            )
    for i in range(1, cols):
        pl.semaphore_signal(
            barrier, inc=1, device_id=(row, (col + i) % cols), device_id_type=MESH
        )
    for i in range(1, rows):
        pl.semaphore_signal(
            barrier, inc=1, device_id=((row + i) % rows, col), device_id_type=MESH
        )
    pl.semaphore_wait(barrier, peers)

    def remote(src, dst, send, recv, target):
        return pltpu.make_async_remote_copy(
            src_ref=src, dst_ref=dst, send_sem=send, recv_sem=recv,
            device_id=target, device_id_type=MESH,
        )

    z_copies = {
        offset: remote(
            z_in, near_z.at[2 - offset], z_send.at[2 + offset], z_recv.at[2 - offset],
            device(me + offset),
        )
        for offset in offsets
    }
    for offset in offsets:
        @pl.when(present(me + offset))
        def _():
            z_copies[offset].start()
    far_copies, part_copies, back_copies, side_copies = [], [], [], []
    for k in range(CHUNKS):
        piece = dosage.at[:, pl.ds(k * width, width)]
        far_copies.append(
            remote(piece, far_raw.at[k], far_send.at[k], far_recv.at[k], device(onward))
        )
        part_copies.append(
            remote(piece, part_raw.at[k], part_send.at[k], part_recv.at[k], device(partner))
        )
        back_copies.append(
            remote(back_out.at[k], back_in.at[k], back_send.at[k], back_recv.at[k], device(source))
        )
        side_copies.append(
            remote(side_out.at[k], side_in.at[k], side_send.at[k], side_recv.at[k], device(partner))
        )
    for k in range(CHUNKS):
        @pl.when(has_onward)
        def _():
            far_copies[k].start()
        part_copies[k].start()

    def gram(left, right):
        product = lax.dot_general(
            left, right, (((0,), (0,)), ((), ())), preferred_element_type=jnp.float32
        )
        return product * (1.0 / samples)

    def keep(flag, tile):
        return jnp.where(flag > 0, tile, jnp.zeros_like(tile)).astype(jnp.bfloat16)

    def span(k):
        return pl.ds(k * width, width)

    def columns(offset, k):
        start = (BAND + offset) * block + k * width
        return pl.ds(pl.multiple_of(start, 128), width)

    def weigh(tile, scores):
        return lax.dot_general(
            scores, tile, (((1,), (1,)), ((), ())), preferred_element_type=jnp.float32
        )

    def tile_at(offset):
        start = (BAND + offset) * block
        return out[:, pl.ds(pl.multiple_of(start, 128), block)]

    flag_far, flag_part, flag_side = flags[0], flags[1], flags[2]
    flag_pair = flags[3]
    flag_back = flags[4]
    own_z = z_in[...]

    for k in range(CHUNKS):
        loads[k].wait()
        own[k] = standardize(raw[k])
    for a in range(CHUNKS):
        for b in range(CHUNKS):
            out[span(a), columns(0, b)] = gram(own[a], own[b]).astype(jnp.bfloat16)
    smoothed = weigh(tile_at(0), own_z)

    for k in range(CHUNKS):
        @pl.when(has_source)
        def _():
            far_copies[k].wait_recv()
        far[k] = standardize(far_raw[k])
        for a in range(CHUNKS):
            back_out[k, :, span(a)] = gram(far[k], own[a]).astype(jnp.bfloat16)
        for a in range(CHUNKS):
            out[span(a), columns(2 * sign, k)] = keep(flag_far, gram(own[a], far[k]))
        @pl.when(has_source)
        def _():
            back_copies[k].start()
        part_copies[k].wait_recv()
        part[k] = standardize(part_raw[k])
        if k < CHUNKS - 1:
            for a in range(CHUNKS):
                out[span(a), columns(sign, k)] = keep(flag_part, gram(own[a], part[k]))
    for k in range(CHUNKS):
        for a in range(CHUNKS):
            side_out[k, span(a), :] = gram(part[a], far[k]).astype(jnp.bfloat16)
        @pl.when(has_source)
        def _():
            side_copies[k].start()
    for a in range(CHUNKS):
        out[span(a), columns(sign, CHUNKS - 1)] = keep(
            flag_part, gram(own[a], part[CHUNKS - 1])
        )

    for offset in offsets:
        @pl.when(present(me + offset))
        def _():
            z_copies[offset].wait_send()
    for offset in offsets:
        @pl.when(present(me - offset))
        def _():
            z_copies[offset].wait_recv()
    far_z, part_z = near_z[BAND + 2 * sign], near_z[BAND + sign]
    part_term = weigh(tile_at(sign), part_z)
    far_term = weigh(tile_at(2 * sign), far_z)
    form = (smoothed + part_term + 2.0 * far_term) * own_z.astype(jnp.float32)
    smoothed = smoothed + part_term + far_term
    pair_term = jnp.zeros_like(smoothed)
    for k in range(CHUNKS):
        tile = side_out[k]
        pair_term = pair_term + weigh(keep(flag_pair, tile), far_z[:, k * width : (k + 1) * width])
    form = form + pair_term * part_z.astype(jnp.float32)
    sum_out[0] = jnp.broadcast_to(jnp.sum(form[0:1], axis=1, keepdims=True), (8, 128))

    col_copies = [
        remote(sum_out.at[0], col_sums.at[i], col_send.at[i], col_recv.at[i], (row, (col + i) % cols))
        for i in range(1, cols)
    ]
    for copy in col_copies:
        copy.start()
    total = sum_out[0]
    for i in range(1, cols):
        col_copies[i - 1].wait()
        total = total + col_sums[i]
    sum_out[1] = total
    row_copies = [
        remote(sum_out.at[1], row_sums.at[i], row_send.at[i], row_recv.at[i], ((row + i) % rows, col))
        for i in range(1, rows)
    ]
    for copy in row_copies:
        copy.start()

    back_z, side_z = near_z[BAND - 2 * sign], near_z[BAND - sign]
    for k in range(CHUNKS):
        @pl.when(has_onward)
        def _():
            back_copies[k].wait_recv()
        start = pl.multiple_of((BAND - 2 * sign) * block, 128)
        out[span(k), pl.ds(start, block)] = keep(flag_back, back_in[k])
    smoothed = smoothed + weigh(tile_at(-2 * sign), back_z)
    for i in range(1, rows):
        row_copies[i - 1].wait()
        total = total + row_sums[i]
    quad[...] = total
    for k in range(CHUNKS):
        @pl.when(has_onward)
        def _():
            side_copies[k].wait_recv()
        out[:, columns(-sign, k)] = keep(flag_side, side_in[k])
    smoothed = smoothed + weigh(tile_at(-sign), side_z)
    smooth[...] = smoothed
    for k in range(CHUNKS):
        @pl.when(has_onward)
        def _():
            far_copies[k].wait_send()
        part_copies[k].wait_send()
        @pl.when(has_source)
        def _():
            back_copies[k].wait_send()
            side_copies[k].wait_send()


def body(rows, cols, dosage, zscores, band_reach):
    samples, block = dosage.shape
    count = rows * cols
    position = lax.axis_index(AXES)
    sign = 1 - 2 * (position % 2)
    width = block // CHUNKS

    def allowed(first, second):
        inside = (first >= 0) & (first < count) & (second >= 0) & (second < count)
        reach = jnp.minimum(
            band_reach[jnp.clip(first, 0, count - 1)], band_reach[jnp.clip(second, 0, count - 1)]
        )
        return (inside & (jnp.abs(first - second) <= reach)).astype(jnp.int32)

    flags = jnp.stack([
        allowed(position, position + 2 * sign),
        allowed(position, position + sign),
        allowed(position, position - sign),
        allowed(position + sign, position + 2 * sign),
        allowed(position, position - 2 * sign),
    ])
    z_rows = jnp.broadcast_to(zscores[None], (ZROWS, block))
    chunked = pltpu.VMEM((CHUNKS, samples, width), jnp.bfloat16)
    vmem = pl.BlockSpec(memory_space=pltpu.VMEM)
    dma = pltpu.SemaphoreType.DMA
    out, smooth, quad = pl.pallas_call(
        functools.partial(kernel, rows, cols),
        out_shape=(
            jax.ShapeDtypeStruct((block, (2 * BAND + 1) * block), jnp.bfloat16),
            jax.ShapeDtypeStruct((ZROWS, block), jnp.float32),
            jax.ShapeDtypeStruct((8, 128), jnp.float32),
        ),
        in_specs=[
            pl.BlockSpec(memory_space=pltpu.SMEM),
            pl.BlockSpec(memory_space=pl.ANY),
            vmem,
        ],
        out_specs=(vmem, vmem, vmem),
        scratch_shapes=[
            chunked, chunked, chunked, chunked, chunked, chunked,
            pltpu.VMEM((CHUNKS, width, block), jnp.bfloat16),
            pltpu.VMEM((CHUNKS, block, width), jnp.bfloat16),
            pltpu.VMEM((CHUNKS, width, block), jnp.bfloat16),
            pltpu.VMEM((CHUNKS, block, width), jnp.bfloat16),
            pltpu.VMEM((2 * BAND + 1, ZROWS, block), jnp.bfloat16),
            pltpu.VMEM((cols, 8, 128), jnp.float32),
            pltpu.VMEM((rows, 8, 128), jnp.float32),
            pltpu.VMEM((2, 8, 128), jnp.float32),
            dma((CHUNKS,)),
            dma((CHUNKS,)), dma((CHUNKS,)), dma((CHUNKS,)), dma((CHUNKS,)),
            dma((CHUNKS,)), dma((CHUNKS,)), dma((CHUNKS,)), dma((CHUNKS,)),
            dma((2 * BAND + 1,)), dma((2 * BAND + 1,)),
            dma((cols,)), dma((cols,)), dma((rows,)), dma((rows,)),
        ],
        compiler_params=pltpu.CompilerParams(
            collective_id=0, has_side_effects=True, vmem_limit_bytes=60 * 1024 * 1024
        ),
    )(flags, dosage, z_rows)
    quadratic = quad[0, 0] / (count * block)
    return (out, smooth[0], quadratic)


def solution(mesh):
    placed = (P(None, AXES), P(AXES), P())
    rows, cols = (mesh.shape[name] for name in AXES)
    return jax.shard_map(
        functools.partial(body, rows, cols),
        mesh=mesh,
        in_specs=placed,
        out_specs=(P(AXES, None), P(AXES), P()),
        check_vma=False,
    )
```

```python
import functools

import jax
import jax.numpy as jnp
from jax import lax
from jax.experimental import pallas as pl
from jax.experimental.pallas import tpu as pltpu
from jax.sharding import PartitionSpec as P

BAND = 2
AXES = ("row", "col")
CHUNKS = 3
ZROWS = 16
MESH = pl.DeviceIdType.MESH


def standardize(chunk):
    values = chunk.astype(jnp.float32)
    column_mean = jnp.mean(values, axis=0, keepdims=True)
    centered = values - column_mean
    variance = jnp.mean(centered * centered, axis=0, keepdims=True)
    return (centered * lax.rsqrt(variance + 1e-05)).astype(jnp.bfloat16)


def kernel(
    rows, cols, reach, dosage, z_in, result, smooth, quad,
    out, raw, far_raw, part_raw, own, far, part, back_out, side_out, back_in, side_in,
    near_z, col_sums, row_sums, sum_out,
    local_sem, far_send, far_recv, part_send, part_recv, back_send, back_recv,
    side_send, side_recv, panel_sem, z_send, z_recv, col_send, col_recv, row_send, row_recv,
):
    samples, block = dosage.shape
    width = block // CHUNKS
    count = rows * cols
    row, col = lax.axis_index("row"), lax.axis_index("col")
    me = row * cols + col
    sign = 1 - 2 * (me % 2)

    def device(index):
        return (index // cols, index % cols)

    def present(index):
        return (index >= 0) & (index < count)

    onward, source, partner = me - 2 * sign, me + 2 * sign, me + sign
    has_onward, has_source = present(onward), present(source)
    offsets = (-2, -1, 1, 2)

    loads = []
    for k in range(CHUNKS):
        load = pltpu.make_async_copy(
            dosage.at[:, pl.ds(k * width, width)], raw.at[k], local_sem.at[k]
        )
        load.start()
        loads.append(load)
    near_z[...] = jnp.zeros_like(near_z)
    near_z[BAND] = jnp.broadcast_to(z_in[...], near_z.shape[1:])

    barrier = pltpu.get_barrier_semaphore()
    peers = cols - 1 + rows - 1
    for offset in offsets:
        outside = present(me + offset) & ((me + offset) // cols != row)
        peers = peers + jnp.where(outside, 1, 0)
        @pl.when(outside)
        def _():
            pl.semaphore_signal(
                barrier, inc=1, device_id=device(me + offset), device_id_type=MESH
            )
    for i in range(1, cols):
        pl.semaphore_signal(
            barrier, inc=1, device_id=(row, (col + i) % cols), device_id_type=MESH
        )
    for i in range(1, rows):
        pl.semaphore_signal(
            barrier, inc=1, device_id=((row + i) % rows, col), device_id_type=MESH
        )
    pl.semaphore_wait(barrier, peers)

    def remote(src, dst, send, recv, target):
        return pltpu.make_async_remote_copy(
            src_ref=src, dst_ref=dst, send_sem=send, recv_sem=recv,
            device_id=target, device_id_type=MESH,
        )

    z_copies = {
        offset: remote(
            near_z.at[BAND], near_z.at[2 - offset], z_send.at[2 + offset], z_recv.at[2 - offset],
            device(me + offset),
        )
        for offset in offsets
    }
    for offset in offsets:
        @pl.when(present(me + offset))
        def _():
            z_copies[offset].start()
    far_copies, part_copies, back_copies, side_copies = [], [], [], []
    for k in range(CHUNKS):
        piece = dosage.at[:, pl.ds(k * width, width)]
        far_copies.append(
            remote(piece, far_raw.at[k], far_send.at[k], far_recv.at[k], device(onward))
        )
        part_copies.append(
            remote(piece, part_raw.at[k], part_send.at[k], part_recv.at[k], device(partner))
        )
        back_copies.append(
            remote(back_out.at[k], back_in.at[k], back_send.at[k], back_recv.at[k], device(source))
        )
        side_copies.append([
            remote(
                side_out.at[k, b], side_in.at[k, b], side_send.at[k, b], side_recv.at[k, b],
                device(partner),
            )
            for b in range(CHUNKS)
        ])
    for k in range(CHUNKS):
        @pl.when(has_onward)
        def _():
            far_copies[k].start()
        part_copies[k].start()

    def gram(left, right):
        product = lax.dot_general(
            left, right, (((0,), (0,)), ((), ())), preferred_element_type=jnp.float32
        )
        return product * (1.0 / samples)

    def keep(flag, tile):
        return jnp.where(flag, tile, jnp.zeros_like(tile)).astype(jnp.bfloat16)

    def span(k):
        return pl.ds(k * width, width)

    def columns(offset, k):
        start = (BAND + offset) * block + k * width
        return pl.ds(pl.multiple_of(start, 128), width)

    def weigh(tile, scores):
        return lax.dot_general(
            scores, tile, (((1,), (1,)), ((), ())), preferred_element_type=jnp.float32
        )

    def tile_at(offset):
        start = (BAND + offset) * block
        return out[:, pl.ds(pl.multiple_of(start, 128), block)]

    def allowed(first, second):
        lowest = jnp.minimum(
            reach[jnp.clip(first, 0, count - 1)], reach[jnp.clip(second, 0, count - 1)]
        )
        return present(first) & present(second) & (jnp.abs(first - second) <= lowest)

    flag_far, flag_part = allowed(me, source), allowed(me, partner)
    flag_back, flag_side = allowed(me, onward), allowed(me, me - sign)
    flag_pair = allowed(partner, source)
    own_z = near_z[BAND]
    panels = []

    def write_panel(offset):
        start = pl.multiple_of((BAND + offset) * block, 128)
        place = pl.ds(start, block)
        panel = pltpu.make_async_copy(
            out.at[:, place], result.at[:, place], panel_sem.at[len(panels)]
        )
        panel.start()
        panels.append(panel)

    for k in range(CHUNKS):
        loads[k].wait()
        own[k] = standardize(raw[k])
    for a in range(CHUNKS):
        for b in range(CHUNKS):
            out[span(a), columns(0, b)] = gram(own[a], own[b]).astype(jnp.bfloat16)
    smoothed = weigh(tile_at(0), own_z)
    write_panel(0)

    for k in range(CHUNKS):
        @pl.when(has_source)
        def _():
            far_copies[k].wait_recv()
        far[k] = standardize(far_raw[k])
        for a in range(CHUNKS):
            back_out[k, :, span(a)] = gram(far[k], own[a]).astype(jnp.bfloat16)
        @pl.when(has_source)
        def _():
            back_copies[k].start()
        part_copies[k].wait_recv()
        part[k] = standardize(part_raw[k])
        blocks = [(a, k) for a in range(k + 1)] + [(k, b) for b in range(k)]
        for a, b in blocks:
            side_out[a, b] = gram(part[a], far[b]).astype(jnp.bfloat16)
            @pl.when(has_source)
            def _():
                side_copies[a][b].start()
        for a in range(CHUNKS):
            out[span(a), columns(2 * sign, k)] = keep(flag_far, gram(own[a], far[k]))
            out[span(a), columns(sign, k)] = keep(flag_part, gram(own[a], part[k]))
    write_panel(2 * sign)
    write_panel(sign)

    for offset in offsets:
        @pl.when(present(me + offset))
        def _():
            z_copies[offset].wait_send()
    for offset in offsets:
        @pl.when(present(me - offset))
        def _():
            z_copies[offset].wait_recv()
    far_z, part_z = near_z[BAND + 2 * sign], near_z[BAND + sign]
    part_term = weigh(tile_at(sign), part_z)
    far_term = weigh(tile_at(2 * sign), far_z)
    form = (smoothed + part_term + 2.0 * far_term) * own_z.astype(jnp.float32)
    smoothed = smoothed + part_term + far_term
    form_sum = jnp.sum(form[0:1], axis=1, keepdims=True)
    for a in range(CHUNKS):
        pair_term = jnp.zeros((ZROWS, width), jnp.float32)
        for b in range(CHUNKS):
            scores = far_z[:, b * width : (b + 1) * width]
            pair_term = pair_term + weigh(keep(flag_pair, side_out[a, b]), scores)
        pair_term = pair_term * part_z[:, a * width : (a + 1) * width].astype(jnp.float32)
        form_sum = form_sum + jnp.sum(pair_term[0:1], axis=1, keepdims=True)
    sum_out[0] = jnp.broadcast_to(form_sum, (8, 128))

    col_copies = [
        remote(sum_out.at[0], col_sums.at[i], col_send.at[i], col_recv.at[i], (row, (col + i) % cols))
        for i in range(1, cols)
    ]
    for copy in col_copies:
        copy.start()
    total = sum_out[0]
    for i in range(1, cols):
        col_copies[i - 1].wait()
        total = total + col_sums[i]
    sum_out[1] = total
    row_copies = [
        remote(sum_out.at[1], row_sums.at[i], row_send.at[i], row_recv.at[i], ((row + i) % rows, col))
        for i in range(1, rows)
    ]
    for copy in row_copies:
        copy.start()

    back_z, side_z = near_z[BAND - 2 * sign], near_z[BAND - sign]
    for k in range(CHUNKS):
        @pl.when(has_onward)
        def _():
            back_copies[k].wait_recv()
        start = pl.multiple_of((BAND - 2 * sign) * block, 128)
        out[span(k), pl.ds(start, block)] = keep(flag_back, back_in[k])
    write_panel(-2 * sign)
    smoothed = smoothed + weigh(tile_at(-2 * sign), back_z)
    for i in range(1, rows):
        row_copies[i - 1].wait()
        total = total + row_sums[i]
    quad[...] = total[0:1, 0:1] / (count * block)
    for k in range(CHUNKS):
        for a, b in [(a, k) for a in range(k + 1)] + [(k, b) for b in range(k)]:
            @pl.when(has_onward)
            def _():
                side_copies[a][b].wait_recv()
            out[span(a), columns(-sign, b)] = keep(flag_side, side_in[a, b])
    write_panel(-sign)
    smoothed = smoothed + weigh(tile_at(-sign), side_z)
    smooth[...] = smoothed[0:1]
    for k in range(CHUNKS):
        @pl.when(has_onward)
        def _():
            far_copies[k].wait_send()
        part_copies[k].wait_send()
        @pl.when(has_source)
        def _():
            back_copies[k].wait_send()
            for b in range(CHUNKS):
                side_copies[k][b].wait_send()
    for panel in panels:
        panel.wait()


def body(rows, cols, dosage, zscores, band_reach):
    samples, block = dosage.shape
    width = block // CHUNKS
    chunked = pltpu.VMEM((CHUNKS, samples, width), jnp.bfloat16)
    vmem = pl.BlockSpec(memory_space=pltpu.VMEM)
    dma = pltpu.SemaphoreType.DMA
    out, smooth, quad = pl.pallas_call(
        functools.partial(kernel, rows, cols),
        out_shape=(
            jax.ShapeDtypeStruct((block, (2 * BAND + 1) * block), jnp.bfloat16),
            jax.ShapeDtypeStruct((1, block), jnp.float32),
            jax.ShapeDtypeStruct((1, 1), jnp.float32),
        ),
        in_specs=[
            pl.BlockSpec(memory_space=pltpu.SMEM),
            pl.BlockSpec(memory_space=pl.ANY),
            vmem,
        ],
        out_specs=(pl.BlockSpec(memory_space=pl.ANY), vmem, vmem),
        scratch_shapes=[
            pltpu.VMEM((block, (2 * BAND + 1) * block), jnp.bfloat16),
            chunked, chunked, chunked, chunked, chunked, chunked,
            pltpu.VMEM((CHUNKS, width, block), jnp.bfloat16),
            pltpu.VMEM((CHUNKS, CHUNKS, width, width), jnp.bfloat16),
            pltpu.VMEM((CHUNKS, width, block), jnp.bfloat16),
            pltpu.VMEM((CHUNKS, CHUNKS, width, width), jnp.bfloat16),
            pltpu.VMEM((2 * BAND + 1, ZROWS, block), jnp.bfloat16),
            pltpu.VMEM((cols, 8, 128), jnp.float32),
            pltpu.VMEM((rows, 8, 128), jnp.float32),
            pltpu.VMEM((2, 8, 128), jnp.float32),
            dma((CHUNKS,)),
            dma((CHUNKS,)), dma((CHUNKS,)), dma((CHUNKS,)), dma((CHUNKS,)),
            dma((CHUNKS,)), dma((CHUNKS,)), dma((CHUNKS, CHUNKS)), dma((CHUNKS, CHUNKS)),
            dma((2 * BAND + 1,)),
            dma((2 * BAND + 1,)), dma((2 * BAND + 1,)),
            dma((cols,)), dma((cols,)), dma((rows,)), dma((rows,)),
        ],
        compiler_params=pltpu.CompilerParams(
            collective_id=0, has_side_effects=True, vmem_limit_bytes=60 * 1024 * 1024
        ),
    )(band_reach, dosage, zscores.reshape(1, block))
    return (out, smooth.reshape(block), quad.reshape(()))


def solution(mesh):
    placed = (P(None, AXES), P(AXES), P())
    rows, cols = (mesh.shape[name] for name in AXES)
    return jax.shard_map(
        functools.partial(body, rows, cols),
        mesh=mesh,
        in_specs=placed,
        out_specs=(P(AXES, None), P(AXES), P()),
        check_vma=False,
    )
```
